256 devices in a mesh: groups: 2 (over y), expert: 128 (over z, x, core).
Axes of the slice: x: 4, y: 2, z: 16, core: 2. Of those that a mesh axis runs over, the one named last changes fastest.
The devices are a block of a 4x16x16 slice.
Arguments:
- tokens: bfloat16 [4096, 3584], P(('groups', 'expert')), parts along dimension 0, may hold values from -6 to 6
- live_counts: int32 [256], P(('groups', 'expert')), parts along dimension 0, may hold values from 8 to 16, as said below
- expert_ids: int32 [4096, 4], P(('groups', 'expert')), parts along dimension 0, may hold values from 0 to 63, all different within a row; in each aligned block of 16 rows (0 to 15, 16 to 31, ...) at most 2 rows name the same one
- gate_scores: float32 [4096, 4], P(('groups', 'expert')), parts along dimension 0, may hold values from 0.1 to 1
- gate_weight: bfloat16 [128, 3584, 512], P('expert'), may hold values from -0.09375 to 0.09375
- up_weight: bfloat16 [128, 3584, 512], P('expert'), may hold values from -0.09375 to 0.09375
- down_weight: bfloat16 [128, 512, 3584], P('expert'), may hold values from -0.1875 to 0.1875
Outputs:
- moe_out: bfloat16 [4096, 3584], P(('groups', 'expert')), parts along dimension 0
The draws below stay inside these ranges and needn't reach their ends.
There are 2 independent parts, one for each index of `groups`. The reference program is written for one: setup_inputs(seed, part) draws one part's arguments, and reference() takes and returns one part's arrays. A program takes and returns all parts, laid end to end along the dimension named above; an argument that names none is the same for every part. Nothing has to cross between parts.
Inputs may be any that keep to these rules, and one draw needn't show every extreme that they name: `expert_ids`: A row names 4 different experts. In each device's aligned block of 16 rows no expert is named by more than 2 rows, a bound that some block reaches. `live_counts`: some device has all 16 slots live.
All inputs are finite; a program needn't handle non-finite values.
Results may differ from the reference program's by a relative error of at most 0.0068.
Values may be sent and summed in bfloat16 or wider, within the bound.
A program may use at most 64 MiB of HBM per device.

```python
import math
import jax
import jax.numpy as jnp
import numpy as np
from jax import lax

D = 3584
FF = 1024
TOP = 4
TOK_DEV = 16
FF_HALF = 512
EXPERTS = 64
CAP = 2
TOKENS = 2048
N_EXPERT = 128


def draw_live_counts(key, part):
    devices = TOKENS // TOK_DEV
    counts = jax.random.randint(jax.random.fold_in(key, 11), (devices,), TOK_DEV // 2, TOK_DEV + 1)
    full_device = jax.random.randint(jax.random.fold_in(key, 12), (), 0, devices)
    counts = jnp.where(jnp.arange(devices) == full_device, TOK_DEV, counts)
    return counts.astype(jnp.int32)


def block_scale(key, extent, pieces, least, largest):
    level, own = 1.0, jax.random.fold_in(key, 6)
    for dim, shards_of in pieces:
        heights = jnp.exp(jax.random.uniform(jax.random.fold_in(own, dim), (shards_of,), jnp.float32, least / len(pieces), largest / len(pieces)))
        level = level * jnp.repeat(heights, extent[dim] // shards_of).reshape([-1 if axis == dim else 1 for axis in range(len(extent))])
    return level


def shared_out(rng, own, number, rows, amount, top, most, slope):
    order = jax.random.permutation(rng, amount)
    packed, usual = portions_of(amount, rows * top, most, slope, True), portions_of(amount, rows * top, most, slope, False)
    places = jnp.arange(amount)

    def named(sizes, turn):
        used = int((sizes > 0).sum())
        fixed = max(1, used // 4)
        passed = fixed + (places - fixed + turn * (used - fixed)) % max(1, amount - fixed)
        return jnp.zeros((amount,), jnp.int32).at[order[jnp.where(places < fixed, places, passed)]].set(jnp.asarray(sizes, jnp.int32))

    sizes = jnp.where(number % 4 == 0, named(packed, number // 4), named(usual, number - number // 4 - 1))
    mixed = jax.random.permutation(jax.random.fold_in(own, 3), amount)
    giver, receiver = mixed[0:amount // 2 * 2:2], mixed[1:amount // 2 * 2:2]
    margin = jnp.minimum(sizes[giver] - 1, most - sizes[receiver]) // 2
    margin = jnp.where((giver == order[0]) | (receiver == order[0]) | (sizes[receiver] == 0), 0, jnp.maximum(margin, 0))
    passed = jax.random.randint(jax.random.fold_in(own, 4), (amount // 2,), 0, 1 << 20) % (margin + 1)
    sizes = sizes.at[giver].add(-passed).at[receiver].add(passed)
    items = jnp.searchsorted(jnp.cumsum(sizes), jnp.arange(rows * top), side="right").astype(jnp.int32)
    table = items.reshape(top, rows).T
    table = table[jax.random.permutation(jax.random.fold_in(own, 1), rows)]
    turn = jax.random.randint(jax.random.fold_in(own, 2), (rows, 1), 0, top)
    return jnp.take_along_axis(table, (jnp.arange(top)[None, :] + turn) % top, axis=1)


def portions_of(number_of, total, most, lean, full):
    portions = [(1 << 20) // math.isqrt(standing ** lean) + 1 for standing in range(1, number_of + 1)]
    largest = most if full else min(most, max(-(-total // number_of), total * portions[0] // sum(portions)))
    least = 1 if total - largest >= number_of - 1 else 0
    given, surplus = [largest] + [least] * (number_of - 1), total - largest - least * (number_of - 1)
    while surplus > 0:
        candidates = [i for i in range(1, number_of) if given[i] < largest] or [i for i in range(1, number_of) if given[i] < most]
        pool, left = sum([portions[i] for i in candidates]), surplus
        for i in candidates:
            addition = min(most - given[i], max(1, left * portions[i] // pool), surplus)
            given[i] = given[i] + addition
            surplus = surplus - addition
    return np.array(given)


def noise(own_key, extent, width, limit, pieces=(), kind=jnp.bfloat16):
    gain = block_scale(own_key, extent, pieces, -0.22, 0.18) if pieces else 1.0
    result = jax.random.normal(own_key, extent, jnp.float32) * width * gain
    return jnp.minimum(jnp.maximum(result, -limit), limit).astype(kind)


def setup_inputs(seed: int = 0, part: int = 0) -> dict:
    key_list = jax.random.split(jax.random.key(seed), 8)
    part_splits = jax.random.split(jax.random.fold_in(key_list[7], part), 8)
    tokens = noise(part_splits[0], (TOKENS, D), 1.0, 6.0, ((0, 128),))
    live_counts = draw_live_counts(jax.random.fold_in(jax.random.fold_in(key_list[7], part), 71), part)
    expert_ids_keys = jax.random.split(jax.random.fold_in(part_splits[2], 1), TOKENS // TOK_DEV)
    expert_ids_turns = jax.random.permutation(jax.random.fold_in(part_splits[2], 3), TOKENS // TOK_DEV)
    expert_ids = jax.vmap(lambda own, number: shared_out(jax.random.fold_in(part_splits[2], 2), own, number, TOK_DEV, EXPERTS, TOP, CAP, 2))(expert_ids_keys, expert_ids_turns).reshape((TOKENS, TOP))
    gate_scores = jnp.clip(jnp.exp(math.log(1.0) - 2.3025851 * jax.random.uniform(part_splits[3], (TOKENS, TOP), jnp.float32) ** block_scale(part_splits[3], (TOKENS, TOP), ((0, 128),), -0.2, 0.2)), 0.1, 1.0)
    gate_weight = noise(key_list[4], (N_EXPERT, D, FF_HALF), D ** -0.5, 0.09375, ((0, 128),))
    up_weight = noise(key_list[5], (N_EXPERT, D, FF_HALF), D ** -0.5, 0.09375, ((0, 128),))
    down_weight = noise(key_list[6], (N_EXPERT, FF_HALF, D), FF ** -0.5, 0.1875, ((0, 128),))
    return dict(tokens=tokens, live_counts=live_counts, expert_ids=expert_ids, gate_scores=gate_scores, gate_weight=gate_weight, up_weight=up_weight, down_weight=down_weight)


def expert_rows(gate_pair, up_pair, down_pair, inputs):
    gate_full = jnp.concatenate([gate_pair[0], gate_pair[1]], axis=1)
    up_full = jnp.concatenate([up_pair[0], up_pair[1]], axis=1)
    down_full = jnp.concatenate([down_pair[0], down_pair[1]], axis=0)
    gate_act = jnp.dot(inputs, gate_full, preferred_element_type=jnp.float32)
    up_act = jnp.dot(inputs, up_full, preferred_element_type=jnp.float32)
    hidden = (jax.nn.silu(gate_act) * up_act).astype(jnp.bfloat16)
    return jnp.dot(hidden, down_full, preferred_element_type=jnp.float32).astype(jnp.bfloat16)


def reference(tokens, live_counts, expert_ids, gate_scores, gate_weight, up_weight, down_weight):
    devices = N_EXPERT
    block_ids = expert_ids.reshape(devices, TOK_DEV * TOP)
    onehot = (block_ids[:, :, None] == jnp.arange(EXPERTS, dtype=jnp.int32)[None, None, :]).astype(jnp.int32)
    earlier = jnp.cumsum(onehot, axis=1) - onehot
    slot_index = jnp.sum(earlier * onehot, axis=2)
    source = jnp.arange(devices, dtype=jnp.int32)[:, None]
    position = (source * CAP + slot_index).reshape(-1).astype(jnp.int32)
    token_index = jnp.repeat(jnp.arange(TOKENS, dtype=jnp.int32), TOP)
    flat_ids = expert_ids.reshape(-1).astype(jnp.int32)
    slot_table = jnp.full((EXPERTS, devices * CAP), TOKENS, dtype=jnp.int32)
    slot_table = slot_table.at[flat_ids, position].set(token_index)
    padded = jnp.concatenate([tokens, jnp.zeros((1, D), tokens.dtype)], axis=0)

    def one_expert(items):
        gate_pair, up_pair, down_pair, table_row = items
        return expert_rows(gate_pair, up_pair, down_pair, padded[table_row])

    results = lax.map(one_expert, (gate_weight.reshape(EXPERTS, 2, D, FF_HALF),
                                   up_weight.reshape(EXPERTS, 2, D, FF_HALF),
                                   down_weight.reshape(EXPERTS, 2, FF_HALF, D),
                                   slot_table))
    picked = results[flat_ids, position].reshape(TOKENS, TOP, D).astype(jnp.float32)
    weighted = jnp.sum(picked * gate_scores[:, :, None].astype(jnp.float32), axis=1)
    local_pos = jnp.arange(TOKENS, dtype=jnp.int32) % TOK_DEV
    live_mask = local_pos < jnp.repeat(live_counts, TOK_DEV)
    return jnp.where(live_mask[:, None], weighted, jnp.zeros_like(weighted)).astype(jnp.bfloat16)
```

```python
import functools

import jax
import jax.numpy as jnp
from jax import lax
from jax.experimental import pallas as pl
from jax.experimental.pallas import tpu as pltpu
from jax.sharding import PartitionSpec as P

MESH = pl.DeviceIdType.MESH
X_CHIPS = 4
CORES = 2
SLOTS = 2
PIECES = 7
PER_ROUND = 4
LANES = 128
F32 = jnp.float32
BF16 = jnp.bfloat16


def routing(ids_ref, scores_ref, live, tok_dev):
    top = ids_ref.shape[0]
    lane = lax.broadcasted_iota(jnp.int32, (tok_dev, LANES), 1)
    token = lax.broadcasted_iota(jnp.int32, (tok_dev, LANES), 0)
    row = lax.broadcasted_iota(jnp.int32, (tok_dev, tok_dev), 0)
    col = lax.broadcasted_iota(jnp.int32, (tok_dev, tok_dev), 1)
    ids = ids_ref[...].astype(F32)
    scores = scores_ref[...]
    expert = lax.div(lane, SLOTS).astype(F32)
    chosen = jnp.zeros((tok_dev, LANES), F32)
    weight = jnp.zeros((tok_dev, LANES), F32)
    for k in range(top):
        id_k = jnp.sum(jnp.where(row == col, ids[k : k + 1, :], 0.0), axis=1, keepdims=True)
        score_k = jnp.sum(jnp.where(row == col, scores[k : k + 1, :], 0.0), axis=1, keepdims=True)
        hit = expert == id_k
        chosen = jnp.where(hit, 1.0, chosen)
        weight = jnp.where(hit, score_k, weight)
    earlier = jnp.where(col < row, 1.0, 0.0).astype(BF16)
    rank = jnp.dot(earlier, chosen.astype(BF16), preferred_element_type=F32)
    mine = (rank == lax.rem(lane, SLOTS).astype(F32)) & (token < live)
    return jnp.where(mine, weight, 0.0)


def kernel(
    planes,
    tokens_ref, live_ref, ids_ref, scores_ref, gate_ref, up_ref, down_ref,
    out_ref,
    head, tail, xout, xin, hidden, yout, yin, contrib, rs_in, rs_out, wg, wu, wd,
    load_sem, w_sem, w_send, w_recv, ag_send, ag_recv, x_send, x_recv, y_send, y_recv,
    rs_send, rs_recv,
):
    tok_dev, width = tokens_ref.shape
    ff_half = gate_ref.shape[2]
    piece = width // PIECES
    half = planes // 2
    cut = (PIECES + 1) // 2
    block = PER_ROUND * SLOTS
    rounds = planes // PER_ROUND
    order = [0]
    for d in range(1, half):
        order += [d, planes - d]
    order.append(half)

    me = lax.axis_index("expert")
    core = lax.rem(me, CORES)
    x = lax.rem(lax.div(me, CORES), X_CHIPS)
    z = lax.div(me, CORES * X_CHIPS)

    def at(z_of, x_of):
        return (z_of * X_CHIPS + x_of) * CORES + core

    above = at(lax.rem(z + 1, planes), x)
    below = at(lax.rem(z + planes - 1, planes), x)
    other = me + 1 - 2 * core
    ahead = [at(z, lax.rem(x + dx, X_CHIPS)) for dx in range(X_CHIPS)]
    behind = [at(z, lax.rem(x + X_CHIPS - dx, X_CHIPS)) for dx in range(X_CHIPS)]

    def remote(src, dst, send, recv, device):
        return pltpu.make_async_remote_copy(
            src_ref=src, dst_ref=dst, send_sem=send, recv_sem=recv,
            device_id={"expert": device}, device_id_type=MESH,
        )

    barrier = pltpu.get_barrier_semaphore()
    peers = [above, below, other] + ahead[1:]
    for peer in peers:
        pl.semaphore_signal(barrier, inc=1, device_id={"expert": peer}, device_id_type=MESH)

    loads = [
        pltpu.make_async_copy(
            tokens_ref.at[:, pl.ds(0, piece)], head.at[0, :, pl.ds(2 * LANES, piece)], load_sem.at[0]
        )
    ]
    for k in range(1, PIECES):
        loads.append(
            pltpu.make_async_copy(
                tokens_ref.at[:, pl.ds(k * piece, piece)], tail.at[0, k - 1], load_sem.at[k]
            )
        )
    for load in loads:
        load.start()
    weights = [(gate_ref, wg), (up_ref, wu), (down_ref, wd)]
    own_weights = [
        pltpu.make_async_copy(src.at[0], dst.at[0], w_sem.at[i]) for i, (src, dst) in enumerate(weights)
    ]
    other_weights = [
        remote(src.at[0], dst.at[1], w_send.at[i], w_recv.at[i], other)
        for i, (src, dst) in enumerate(weights)
    ]
    table = routing(ids_ref, scores_ref, live_ref[0], tok_dev)
    table_high = table.astype(BF16)
    head[0, :, 0:LANES] = table_high
    head[0, :, LANES : 2 * LANES] = (table - table_high.astype(F32)).astype(BF16)

    def chunk(q, k):
        return head.at[q] if isinstance(k, int) and k == 0 else tail.at[q, k - 1]

    def pass_up(q, k):
        return remote(chunk(q, k), chunk(q + 1, k), ag_send.at[q, k], ag_recv.at[q + 1, k], above)

    def pass_down(q, k):
        at_q = half if q == 0 else q
        to = planes - 1 if q == 0 else q - 1
        return remote(chunk(q, k), chunk(to, k), ag_send.at[at_q, k], ag_recv.at[to, k], below)

    def take(q, k):
        remote(chunk(q, k), chunk(q, k), ag_send.at[q, k], ag_recv.at[q, k], above).wait_recv()

    pl.semaphore_wait(barrier, len(peers))
    for k in range(PIECES):
        loads[k].wait()
        pass_up(0, k).start()
        pass_down(0, k).start()
    for i in range(len(weights)):
        other_weights[i].start()
        own_weights[i].start()

    rows = X_CHIPS * block
    lane_of = lax.broadcasted_iota(jnp.int32, (LANES, rows), 0)
    row_of = lax.broadcasted_iota(jnp.int32, (LANES, rows), 1)
    chip_of = lax.rem(x + lax.div(row_of, block), X_CHIPS)
    wanted = (z * X_CHIPS + chip_of) * SLOTS + lax.rem(row_of, SLOTS)
    select = jnp.where(lane_of == wanted, 1.0, 0.0).astype(BF16)
    flat = PER_ROUND * tok_dev
    plane_a = lax.div(lax.broadcasted_iota(jnp.int32, (flat, rows), 0), tok_dev)
    plane_b = lax.rem(lax.div(lax.broadcasted_iota(jnp.int32, (flat, rows), 1), SLOTS), PER_ROUND)
    same_plane = plane_a == plane_b

    def of_round(r):
        return order[r * PER_ROUND : (r + 1) * PER_ROUND]

    def picked(r, low):
        part = jnp.concatenate([head[q, :, low * LANES : (low + 1) * LANES] for q in of_round(r)], axis=0)
        return part

    def x_copy(r, dx):
        return remote(
            xout.at[r, dx - 1], xin.at[r * X_CHIPS + dx], x_send.at[r, dx - 1], x_recv.at[r, dx - 1],
            ahead[dx],
        )

    def pack(r):
        used = jnp.where(picked(r, 0).astype(F32) != 0.0, 1.0, 0.0).astype(BF16)
        place = jnp.dot(used, select, preferred_element_type=F32)
        place = jnp.where(same_plane, place, 0.0).astype(BF16)
        for k in range(PIECES):
            if k == 0:
                parts = [head[q, :, 2 * LANES :] for q in of_round(r)]
            else:
                parts = [tail[q, k - 1] for q in of_round(r)]
            packed = lax.dot_general(
                place, jnp.concatenate(parts, axis=0), (((0,), (0,)), ((), ())),
                preferred_element_type=F32,
            )
            cols = slice(k * piece, (k + 1) * piece)
            xin[r * X_CHIPS, :, cols] = packed[0:block].astype(BF16)
            for dx in range(1, X_CHIPS):
                xout[r, dx - 1, :, cols] = packed[dx * block : (dx + 1) * block].astype(BF16)
        for dx in range(1, X_CHIPS):
            x_copy(r, dx).start()

    packed_rounds = 0
    for d in range(1, half):
        up_q, down_q = d, planes - d
        if d + 1 < half:
            take(up_q, 0)
            pass_up(up_q, 0).start()
            take(down_q, 0)
            pass_down(down_q, 0).start()

            @pl.loop(1, PIECES)
            def _(k):
                take(up_q, k)
                pass_up(up_q, k).start()
                take(down_q, k)
                pass_down(down_q, k).start()
        else:
            for k in range(PIECES):
                take(up_q, k)
                if k < cut:
                    pass_up(up_q, k).start()
                take(down_q, k)
                if k >= cut:
                    pass_down(down_q, k).start()
        while packed_rounds < rounds - 1 and all(
            min(q, planes - q) <= d for q in of_round(packed_rounds)
        ):
            pack(packed_rounds)
            packed_rounds += 1
    for k in range(PIECES):
        take(half, k)
    for r in range(packed_rounds, rounds):
        pack(r)

    for copy in own_weights:
        copy.wait()
    for copy in other_weights:
        copy.wait_recv()
    for r in range(rounds):
        for dx in range(1, X_CHIPS):
            x_copy(r, dx).wait_recv()

    n_rows = rounds * rows
    step = min(256, ff_half)

    for part in range(CORES):

        @pl.loop(0, ff_half // step)
        def _(i):
            cols = pl.ds(pl.multiple_of(i * step, step), step)
            inputs = xin[...].reshape(n_rows, width)
            gate = jnp.dot(inputs, wg[part, :, cols], preferred_element_type=F32)
            up = jnp.dot(inputs, wu[part, :, cols], preferred_element_type=F32)
            hidden[part, :, cols] = (gate / (1.0 + jnp.exp(-gate)) * up).astype(BF16)

    last = rounds - 1

    def y_piece(dx, k):
        cols = pl.ds(k * piece, piece)
        slot = last * X_CHIPS + dx
        return remote(
            yout.at[slot, :, cols], yin.at[slot, :, cols], y_send.at[last + dx - 1, k],
            y_recv.at[last + dx - 1, k], behind[dx],
        )

    def y_copy(r, dx):
        slot = r * X_CHIPS + dx
        return remote(
            yout.at[slot], yin.at[slot], y_send.at[r, dx - 1], y_recv.at[r, dx - 1], behind[dx]
        )

    for k in range(PIECES):
        cols = slice(k * piece, (k + 1) * piece)
        result = jnp.dot(hidden[0], wd[0, :, cols], preferred_element_type=F32)
        result += jnp.dot(hidden[1], wd[1, :, cols], preferred_element_type=F32)
        result = result.reshape(rounds, X_CHIPS, block, piece).astype(BF16)
        for r in range(rounds):
            yin[r * X_CHIPS, :, cols] = result[r, 0]
            for dx in range(1, X_CHIPS):
                yout[r * X_CHIPS + dx, :, cols] = result[r, dx]
        for dx in range(1, X_CHIPS):
            y_piece(dx, k).start()
    for r in range(last - 1, -1, -1):
        for dx in range(1, X_CHIPS):
            y_copy(r, dx).start()

    def weights_of(r, low):
        part = jnp.dot(picked(r, low), select, preferred_element_type=F32)
        return jnp.where(same_plane, part, 0.0).astype(BF16)

    def combine(r, k, high, low):
        cols = slice(k * piece, (k + 1) * piece)
        rows_in = yin[r * X_CHIPS : (r + 1) * X_CHIPS, :, cols].reshape(rows, piece)
        total = jnp.dot(high, rows_in, preferred_element_type=F32)
        total += jnp.dot(low, rows_in, preferred_element_type=F32)
        for j, q in enumerate(of_round(r)):
            contrib[q, k] = total[j * tok_dev : (j + 1) * tok_dev]

    def rs_down(q, k):
        return remote(rs_out.at[q, k], rs_in.at[q - 1, k], rs_send.at[q, k], rs_recv.at[q - 1, k], below)

    def rs_up(q, k):
        return remote(rs_out.at[q, k], rs_in.at[q + 1, k], rs_send.at[q, k], rs_recv.at[q + 1, k], above)

    def rs_take(q, k):
        remote(rs_in.at[q, k], rs_in.at[q, k], rs_recv.at[q, k], rs_recv.at[q, k], above).wait_recv()

    high, low = weights_of(last, 0), weights_of(last, 1)
    for k in range(PIECES):
        for dx in range(1, X_CHIPS):
            y_piece(dx, k).wait_recv()
        combine(last, k, high, low)
        rs_out[half, k] = contrib[half, k].astype(BF16)
        (rs_down if k < cut else rs_up)(half, k).start()

    combined = {last}
    for d in range(half - 1, 0, -1):
        down_q, up_q = d, planes - d
        for q in (down_q, up_q):
            r = order.index(q) // PER_ROUND
            if r not in combined:
                combined.add(r)
                for dx in range(1, X_CHIPS):
                    y_copy(r, dx).wait_recv()
                high, low = weights_of(r, 0), weights_of(r, 1)
                for k in range(PIECES):
                    combine(r, k, high, low)
        if d == half - 1:
            for k in range(PIECES):
                for q, incoming, push in ((down_q, k < cut, rs_down), (up_q, k >= cut, rs_up)):
                    if incoming:
                        rs_take(q, k)
                        rs_out[q, k] = (contrib[q, k] + rs_in[q, k].astype(F32)).astype(BF16)
                    else:
                        rs_out[q, k] = contrib[q, k].astype(BF16)
                    push(q, k).start()
        else:

            @pl.loop(0, PIECES)
            def _(k):
                for q, push in ((down_q, rs_down), (up_q, rs_up)):
                    rs_take(q, k)
                    rs_out[q, k] = (contrib[q, k] + rs_in[q, k].astype(F32)).astype(BF16)
                    push(q, k).start()

    r = 0
    if r not in combined:
        for dx in range(1, X_CHIPS):
            y_copy(r, dx).wait_recv()
        high, low = weights_of(r, 0), weights_of(r, 1)
        for k in range(PIECES):
            combine(r, k, high, low)
    for k in range(PIECES):
        rs_take(0, k)
        rs_take(planes, k)
        total = contrib[0, k] + rs_in[0, k].astype(F32) + rs_in[planes, k].astype(F32)
        out_ref[:, k * piece : (k + 1) * piece] = total.astype(BF16)

    for copy in other_weights:
        copy.wait_send()
    for k in range(PIECES):
        pass_up(0, k).wait_send()
        pass_down(0, k).wait_send()
    for d in range(1, half):
        for k in range(PIECES):
            if d + 1 < half or k < cut:
                pass_up(d, k).wait_send()
            if d + 1 < half or k >= cut:
                pass_down(planes - d, k).wait_send()
    for r in range(rounds):
        for dx in range(1, X_CHIPS):
            x_copy(r, dx).wait_send()
            if r < last:
                y_copy(r, dx).wait_send()
    for k in range(PIECES):
        for dx in range(1, X_CHIPS):
            y_piece(dx, k).wait_send()
        (rs_down if k < cut else rs_up)(half, k).wait_send()
        for d in range(1, half):
            rs_down(d, k).wait_send()
            rs_up(planes - d, k).wait_send()


def shards(tokens, live_counts, expert_ids, gate_scores, gate_weight, up_weight, down_weight):
    tok_dev, width = tokens.shape
    ff_half = gate_weight.shape[2]
    planes = lax.axis_size("expert") // (X_CHIPS * CORES)
    rounds = planes // PER_ROUND
    piece = width // PIECES
    block = PER_ROUND * SLOTS
    slots = rounds * X_CHIPS
    vmem, dma = pltpu.VMEM, pltpu.SemaphoreType.DMA
    scratch = [
        vmem((planes, tok_dev, 2 * LANES + piece), BF16),
        vmem((planes, PIECES - 1, tok_dev, piece), BF16),
        vmem((rounds, X_CHIPS - 1, block, width), BF16),
        vmem((slots, block, width), BF16),
        vmem((CORES, slots * block, ff_half), BF16),
        vmem((slots, block, width), BF16),
        vmem((slots, block, width), BF16),
        vmem((planes, PIECES, tok_dev, piece), F32),
        vmem((planes + 1, PIECES, tok_dev, piece), BF16),
        vmem((planes, PIECES, tok_dev, piece), BF16),
        vmem((CORES, width, ff_half), BF16),
        vmem((CORES, width, ff_half), BF16),
        vmem((CORES, ff_half, width), BF16),
        dma((PIECES,)),
        dma((3,)),
        dma((3,)),
        dma((3,)),
        dma((planes, PIECES)),
        dma((planes, PIECES)),
        dma((rounds, X_CHIPS - 1)),
        dma((rounds, X_CHIPS - 1)),
        dma((rounds + X_CHIPS - 2, PIECES)),
        dma((rounds + X_CHIPS - 2, PIECES)),
        dma((planes, PIECES)),
        dma((planes + 1, PIECES)),
    ]
    in_vmem = pl.BlockSpec(memory_space=pltpu.VMEM)
    in_smem = pl.BlockSpec(memory_space=pltpu.SMEM)
    anywhere = pl.BlockSpec(memory_space=pl.ANY)
    return pl.pallas_call(
        functools.partial(kernel, planes),
        out_shape=jax.ShapeDtypeStruct((tok_dev, width), BF16),
        in_specs=[anywhere, in_smem, in_vmem, in_vmem, anywhere, anywhere, anywhere],
        out_specs=in_vmem,
        scratch_shapes=scratch,
        compiler_params=pltpu.CompilerParams(
            collective_id=0, has_side_effects=True, vmem_limit_bytes=60 * 1024 * 1024
        ),
        name="moe_layer",
    )(tokens, live_counts, expert_ids.T, gate_scores.T, gate_weight, up_weight, down_weight)


def solution(mesh):
    both = P(("groups", "expert"), None)
    weight = P("expert", None, None)
    in_specs = (both, P(("groups", "expert")), both, both, weight, weight, weight)
    return jax.shard_map(shards, mesh=mesh, in_specs=in_specs, out_specs=both, check_vma=False)
```
